32 devices in a mesh: dp: 8 (over z, x), tp: 4 (over y, core).
Axes of the slice: x: 2, y: 2, z: 4, core: 2. Of those that a mesh axis runs over, the one named last changes fastest.
Arguments:
- slopes: bfloat16 [8, 2, 3072, 768], P('dp', None, 'tp'), may hold values from -6 to 6, as said below
- basis_in: float32 [2, 768, 8], replicated, may hold values from -6 to 6
- weights_in: float32 [2, 3072, 768], P(None, 'tp', 'dp'), may hold values from -0.21875 to 0.21875
Outputs:
- new_weights: float32 [2, 3072, 768], P(None, 'tp', 'dp')
- new_basis: float32 [2, 768, 8], replicated
The draws below stay inside these ranges and needn't reach their ends.
Inputs may be any that keep to these rules, and one draw needn't show every extreme that they name: slopes holds numbers from -6 to 6.
All inputs are finite; a program needn't handle non-finite values.
Results may differ from the reference program's by a relative error of at most 0.0003.
Values sent between devices are 32-bit elements.
A program may use at most 64 MiB of HBM per device.

```python
import jax
import jax.numpy as jnp
from jax import lax

WIDTH = 768
INNER = 3072
RANK = 8
LAYERS = 2
REPLICAS = 8
N_TP = 4


def draw_slopes(key, part):
    keys = jax.random.split(key, 5)
    level = jnp.exp(jax.random.uniform(keys[4], (1, LAYERS, N_TP, 1, RANK), jnp.float32, -1.3, 1.3))
    left = jax.random.normal(keys[0], (1, LAYERS, N_TP, INNER // N_TP, RANK), jnp.float32) * level
    left = left.reshape(1, LAYERS, INNER, RANK)
    right = jax.random.normal(keys[1], (1, LAYERS, RANK, WIDTH), jnp.float32)
    strength = jax.random.normal(keys[2], (REPLICAS, LAYERS, 1, RANK), jnp.float32)
    noise = jax.random.normal(keys[3], (REPLICAS, LAYERS, INNER, WIDTH), jnp.float32)
    low = jnp.einsum('alir,lrw->aliw', left * strength, right[0])
    values = low * RANK ** (-0.5) + 0.5 * noise
    return jnp.clip(values, -6.0, 6.0).astype(jnp.bfloat16)


def shard_levels(rng, dims, shards, low, high):
    factor_of = 1.0
    for axis_at, blocks in shards:
        steps = jax.random.uniform(jax.random.fold_in(jax.random.fold_in(rng, 6), axis_at), (blocks,), jnp.float32, low / len(shards), high / len(shards))
        factor_of = factor_of * jnp.repeat(jnp.exp(steps), dims[axis_at] // blocks).reshape((-1,) + (1,) * (len(dims) - 1 - axis_at))
    return factor_of


def bell_draw(rng, shape, scale, limit, shards=(), kind=jnp.bfloat16):
    entries = jax.random.normal(rng, shape, jnp.float32) * scale
    if len(shards) > 0:
        entries = shard_levels(rng, shape, shards, -0.22, 0.18) * entries
    return jnp.clip(entries, min=-limit, max=limit).astype(kind)


def setup_inputs(seed: int = 0) -> dict:
    key_of = jax.random.split(jax.random.key(seed), 4)
    slopes = draw_slopes(jax.random.fold_in(key_of[3], 71), 0)
    basis_in = bell_draw(key_of[1], (LAYERS, WIDTH, RANK), 1.0, 6.0, (), jnp.float32)
    weights_in = bell_draw(key_of[2], (LAYERS, INNER, WIDTH), WIDTH ** -0.5, 0.21875, ((1, 4), (2, 8)), jnp.float32)
    return dict(slopes=slopes, basis_in=basis_in, weights_in=weights_in)


def reference(slopes, basis_in, weights_in):
    small_basis = basis_in.astype(jnp.bfloat16)
    small_basis = lax.optimization_barrier(small_basis)
    left = jnp.einsum('aliw,lwr->lir', slopes.astype(jnp.float32), small_basis.astype(jnp.float32))
    gram = jnp.einsum('lir,lis->lrs', left, left, precision=lax.Precision.HIGHEST)
    gram = gram + 0.001 * lax.optimization_barrier(jnp.mean(jnp.diagonal(gram, axis1=1, axis2=2), axis=1))[:, None, None] * jnp.eye(RANK, dtype=jnp.float32)
    small_left = lax.optimization_barrier(left.astype(jnp.bfloat16))
    right = jnp.einsum('aliw,lir->lwr', slopes.astype(jnp.float32), small_left.astype(jnp.float32))
    root = jnp.linalg.cholesky(gram)
    half = lax.linalg.triangular_solve(root, jnp.swapaxes(right, 1, 2), left_side=True, lower=True)
    mixed = lax.linalg.triangular_solve(root, half, left_side=True, lower=True, transpose_a=True)
    change = jnp.einsum('lir,lrw->liw', left, mixed, precision=lax.Precision.HIGHEST) / REPLICAS
    new_weights = weights_in - 0.02 * change
    new_basis = right * lax.rsqrt(lax.optimization_barrier(jnp.mean(right * right, axis=(1, 2), keepdims=True)) + 1e-12)
    return (new_weights, new_basis)
```

```python
import functools

import jax
import jax.numpy as jnp
from jax import lax
from jax.experimental import pallas as pl
from jax.experimental.pallas import tpu as pltpu
from jax.sharding import PartitionSpec as P

MESH = pl.DeviceIdType.MESH
HIGH = lax.Precision.HIGHEST
LANES = 128


def dot(a, b, dims, precision=None):
    return lax.dot_general(
        a, b, ((dims[:1], dims[1:]), ((), ())), precision=precision, preferred_element_type=jnp.float32
    )


def split(x):
    parts = []
    for _ in range(3):
        part = x.astype(jnp.bfloat16).astype(jnp.float32)
        parts.append(part)
        x = x - part
    return parts


def stack(x, order):
    parts = split(x)
    return jnp.concatenate([parts[k] for k in order], axis=0).astype(jnp.bfloat16)


LEFT_ORDER = (0, 0, 1, 0, 2, 1)
RIGHT_ORDER = (0, 1, 0, 2, 0, 1)


def kernel(
    n, m, layers, rank, slopes_ref, basis_ref, weights_ref, out_ref, basis_out_ref,
    slopes, weights, part1, got1, all1, left_ref, part2, got2, tp2, all2, grams,
    in_sem, w_sem, o_sem, s1, r1, s2, r2, s3, r3, s4, r4, s5, r5, s6, r6,
):
    dp = lax.axis_index("dp")
    tp = lax.axis_index("tp")
    dp_peer = [None] + [lax.rem(dp + k, n) for k in range(1, n)]
    tp_peer = [None] + [lax.rem(tp + k, m) for k in range(1, m)]
    rows_all = layers * rank
    depth = slopes.shape[1]
    block = out_ref.shape[1]
    rows, lanes = part1.shape[1:]
    per_row = depth // lanes

    loads = []
    for l in range(layers):
        copy = pltpu.make_async_copy(slopes_ref.at[l], slopes.at[l], in_sem.at[l])
        copy.start()
        loads.append(copy)
    w_load = pltpu.make_async_copy(weights_ref, weights, w_sem)
    w_load.start()

    barrier = pltpu.get_barrier_semaphore()
    for k in range(1, n):
        pl.semaphore_signal(barrier, inc=1, device_id=(dp_peer[k], tp), device_id_type=MESH)
    for k in range(1, m):
        pl.semaphore_signal(barrier, inc=1, device_id=(dp, tp_peer[k]), device_id_type=MESH)

    def dp_copy(src, dst, k, send, recv):
        return pltpu.make_async_remote_copy(
            src_ref=src, dst_ref=dst, send_sem=send.at[k], recv_sem=recv.at[k],
            device_id=(dp_peer[k], tp), device_id_type=MESH,
        )

    def tp_copy(src, dst, k, send, recv):
        return pltpu.make_async_remote_copy(
            src_ref=src, dst_ref=dst, send_sem=send.at[k], recv_sem=recv.at[k],
            device_id=(dp, tp_peer[k]), device_id_type=MESH,
        )

    def place(c):
        row = c // per_row * rows
        lane = c % per_row * lanes
        return slice(row, row + rows), slice(lane, lane + lanes)

    for l in range(layers):
        loads[l].wait()
        left_ref[l * rank:(l + 1) * rank, :] = dot(
            basis_ref[l].astype(jnp.bfloat16), slopes[l], (1, 1)
        )
    for c in range(n):
        at = place(c)
        part1[c] = left_ref[at[0], at[1]]
    pl.semaphore_wait(barrier, n + m - 2)

    sends = [dp_copy(part1.at[dp_peer[k]], got1.at[k], k, s1, r1) for k in range(1, n)]
    for copy in sends:
        copy.start()
    total = part1[dp]
    for k in range(1, n):
        sends[k - 1].wait_recv()
        total = total + got1[k]
    all1[dp] = total
    gathers = [dp_copy(all1.at[dp], all1.at[dp], k, s2, r2) for k in range(1, n)]
    for copy in gathers:
        copy.start()
    for copy in sends:
        copy.wait_send()
    for copy in gathers:
        copy.wait_recv()
    for c in range(n):
        at = place(c)
        left_ref[at[0], at[1]] = all1[c]
    lefts = [left_ref[l * rank:(l + 1) * rank, :] for l in range(layers)]

    for l in range(layers):
        term = dot(lefts[l].astype(jnp.bfloat16), slopes[l], (1, 0))
        for c in range(n):
            part2[c, l * rank:(l + 1) * rank, :] = jnp.concatenate(
                [term[:, c * block:(c + 1) * block], jnp.zeros((rank, LANES - block), jnp.float32)], axis=1
            )
    sends2 = [dp_copy(part2.at[dp_peer[k]], got2.at[k], k, s3, r3) for k in range(1, n)]
    for copy in sends2:
        copy.start()

    own = [dot(left, left, (1, 1), HIGH) for left in lefts]
    grams[tp] = jnp.concatenate(
        own + [jnp.zeros((rank, LANES - layers * rank), jnp.float32)], axis=1
    )
    gram_sends = [tp_copy(grams.at[tp], grams.at[tp], k, s5, r5) for k in range(1, m)]
    for copy in gram_sends:
        copy.start()
    for copy in gathers:
        copy.wait_send()
    for copy in gram_sends:
        copy.wait_recv()
    gram_all = grams[0]
    for k in range(1, m):
        gram_all = gram_all + grams[k]
    row_id = lax.broadcasted_iota(jnp.int32, (rank, rank), 0)
    col_id = lax.broadcasted_iota(jnp.int32, (rank, rank), 1)
    eye = (row_id == col_id).astype(jnp.float32)
    wide_row = lax.broadcasted_iota(jnp.int32, (rank, 2 * rank), 0)
    tables = []
    for l in range(layers):
        gram = gram_all[:, l * rank:(l + 1) * rank]
        mean = jnp.sum(gram * eye, keepdims=True) / rank
        tables.append(jnp.concatenate([gram + 0.001 * mean * eye, eye], axis=1))
    for step in range(rank - 1):
        for l in range(layers):
            table = tables[l]
            factor = table[:, step:step + 1] / table[step:step + 1, step:step + 1]
            change = factor * table[step:step + 1, :]
            tables[l] = table - jnp.where(wide_row > step, change, 0.0)
    solved = []
    for l in range(layers):
        lower = tables[l][:, rank:]
        pivots = jnp.sum(tables[l][:, :rank] * eye, axis=1, keepdims=True)
        half = dot(lower, lefts[l], (1, 0), HIGH) / pivots
        full = dot(lower, half, (0, 0), HIGH) * (0.02 / n)
        solved.append(stack(full, LEFT_ORDER))

    total = part2[dp]
    for k in range(1, n):
        sends2[k - 1].wait_recv()
        total = total + got2[k]
    tp2[tp] = total
    tp_sends = [tp_copy(tp2.at[tp], tp2.at[tp], k, s4, r4) for k in range(1, m)]
    for copy in tp_sends:
        copy.start()
    for copy in sends2:
        copy.wait_send()
    for copy in tp_sends:
        copy.wait_recv()
    total = tp2[0]
    for k in range(1, m):
        total = total + tp2[k]
    all2[dp] = total
    gathers2 = [dp_copy(all2.at[dp], all2.at[dp], k, s6, r6) for k in range(1, n)]
    for copy in gathers2:
        copy.start()

    w_load.wait()
    outs = []
    for l in range(layers):
        mine = stack(total[l * rank:(l + 1) * rank, :], RIGHT_ORDER)
        change = dot(mine, solved[l], (0, 0))
        weights[l] = weights[l] - change[:block, :]
        copy = pltpu.make_async_copy(weights.at[l], out_ref.at[l], o_sem.at[l])
        copy.start()
        outs.append(copy)

    for copy in gram_sends + tp_sends:
        copy.wait_send()
    for copy in gathers2:
        copy.wait_recv()
    for l in range(layers):
        pieces = [all2[c, l * rank:(l + 1) * rank, :] for c in range(n)]
        square = pieces[0] * pieces[0]
        for piece in pieces[1:]:
            square = square + piece * piece
        mean = jnp.sum(square, keepdims=True) / (rank * n * block)
        scale = lax.rsqrt(mean + 1e-12)
        for c in range(n):
            basis_out_ref[l, :, c * block:(c + 1) * block] = (pieces[c] * scale)[:, :block]
    for copy in gathers2:
        copy.wait_send()
    for copy in outs:
        copy.wait()


def body(slopes, basis_in, weights_in):
    n = lax.axis_size("dp")
    m = lax.axis_size("tp")
    _, layers, depth, width = slopes.shape
    rank = basis_in.shape[2]
    block = weights_in.shape[2]
    total = layers * rank
    rows = max(1, total // n)
    lanes = total * depth // (n * rows)
    f32 = jnp.float32
    dma = pltpu.SemaphoreType.DMA
    any_spec = pl.BlockSpec(memory_space=pl.ANY)
    vmem_spec = pl.BlockSpec(memory_space=pltpu.VMEM)
    new_weights, new_basis = pl.pallas_call(
        functools.partial(kernel, n, m, layers, rank),
        out_shape=(
            jax.ShapeDtypeStruct((layers, block, depth), f32),
            jax.ShapeDtypeStruct((layers, rank, width), f32),
        ),
        in_specs=[any_spec, vmem_spec, any_spec],
        out_specs=(any_spec, vmem_spec),
        scratch_shapes=[
            pltpu.VMEM((layers, depth, width), jnp.bfloat16),
            pltpu.VMEM((layers, block, depth), f32),
            pltpu.VMEM((n, rows, lanes), f32),
            pltpu.VMEM((n, rows, lanes), f32),
            pltpu.VMEM((n, rows, lanes), f32),
            pltpu.VMEM((total, depth), f32),
            pltpu.VMEM((n, total, LANES), f32),
            pltpu.VMEM((n, total, LANES), f32),
            pltpu.VMEM((m, total, LANES), f32),
            pltpu.VMEM((n, total, LANES), f32),
            pltpu.VMEM((m, rank, LANES), f32),
            dma((layers,)), dma, dma((layers,)),
            dma((n,)), dma((n,)), dma((n,)), dma((n,)), dma((n,)), dma((n,)),
            dma((m,)), dma((m,)), dma((m,)), dma((m,)), dma((n,)), dma((n,)),
        ],
        compiler_params=pltpu.CompilerParams(collective_id=0, has_side_effects=True),
    )(slopes[0], jnp.swapaxes(basis_in, 1, 2), jnp.swapaxes(weights_in, 1, 2))
    return jnp.swapaxes(new_weights, 1, 2), jnp.swapaxes(new_basis, 1, 2)


def solution(mesh):
    placed = (P("dp", None, "tp", None), P(), P(None, "tp", "dp"))
    return jax.shard_map(
        body, mesh=mesh, in_specs=placed, out_specs=(P(None, "tp", "dp"), P()), check_vma=False
    )
```
